128 devices in a mesh: tp: 16 (over z, y), dp: 8 (over x, core).
Axes of the slice: x: 4, y: 4, z: 4, core: 2. Of those that a mesh axis runs over, the one named last changes fastest.
Arguments:
- feats: bfloat16 [2048, 36, 1024], P('dp')
- ln_gamma: float32 [1024], replicated
- ln_beta: float32 [1024], replicated
- w_head: bfloat16 [1024, 22528], P(None, 'tp')
- b_head: float32 [22528], P('tp')
- labels: int32 [2048], P('dp')
Outputs:
- output 1: float32 [], replicated
- output 2: bfloat16 [2048, 36, 1024], P('dp')
- output 3: float32 [1024, 22528], P(None, 'tp')
- output 4: float32 [22528], P('tp')
- output 5: float32 [1024], replicated
- output 6: float32 [1024], replicated
All inputs are finite; a program needn't handle non-finite values.
Results may differ from the reference program's by a relative error of at most 0.001.
Values sent between devices are 32-bit elements.
A program may use at most 1 GiB of HBM per device.

```python
import jax
import jax.numpy as jnp
from jax import lax

GLOBAL_BATCH = 2048
TOKENS = 36
WIDTH = 1024
CLASSES = 21841
PADDED_CLASSES = 22528
ROW_BLOCK = min(GLOBAL_BATCH, 64)
LN_EPS = 1e-5
SMOOTH = 0.1


def setup_inputs(seed: int = 0) -> dict:
    sub_keys = jax.random.split(jax.random.key(seed), 7)
    image_shared = jax.random.normal(sub_keys[0], (GLOBAL_BATCH, 1, WIDTH), jnp.float32)
    token_noise = jax.random.normal(sub_keys[1], (GLOBAL_BATCH, TOKENS, WIDTH), jnp.float32)
    feats = (image_shared + 0.5 * token_noise).astype(jnp.bfloat16)
    ln_gamma = 1.0 + 0.3 * jax.random.normal(sub_keys[2], (WIDTH,), jnp.float32)
    ln_beta = 0.3 * jax.random.normal(sub_keys[3], (WIDTH,), jnp.float32)
    w_scale = 3.0 * WIDTH ** -0.5
    w_head = (w_scale * jax.random.normal(sub_keys[4], (WIDTH, PADDED_CLASSES), jnp.float32)).astype(jnp.bfloat16)
    b_head = 0.5 * jax.random.normal(sub_keys[5], (PADDED_CLASSES,), jnp.float32)
    labels = jax.random.randint(sub_keys[6], (GLOBAL_BATCH,), 0, CLASSES, dtype=jnp.int32)
    labels = labels.at[0].set(0).at[GLOBAL_BATCH - 1].set(CLASSES - 1)
    return {"feats": feats, "ln_gamma": ln_gamma, "ln_beta": ln_beta, "w_head": w_head, "b_head": b_head, "labels": labels}


def norm_pool(feats, ln_gamma, ln_beta):
    x_val = feats.astype(jnp.float32)
    mean_x = jnp.mean(x_val, axis=-1, keepdims=True)
    centered = x_val - mean_x
    var_x = jnp.mean(centered * centered, axis=-1, keepdims=True)
    inv_std = lax.rsqrt(var_x + LN_EPS)
    x_hat = centered * inv_std
    x_hat_mean = jnp.mean(x_hat, axis=1)
    pooled16 = (x_hat_mean * ln_gamma + ln_beta).astype(jnp.bfloat16)
    return x_hat, inv_std, x_hat_mean, pooled16


def norm_backward(grad_pool, x_hat, inv_std, x_hat_mean, ln_gamma):
    grad_gamma = jnp.sum(grad_pool * x_hat_mean, axis=0)
    grad_beta = jnp.sum(grad_pool, axis=0)
    upstream = grad_pool * ln_gamma / TOKENS
    up_mean = jnp.mean(upstream, axis=-1)
    proj_term = jnp.mean(x_hat * upstream[:, None, :], axis=-1, keepdims=True)
    grad_x = inv_std * (upstream[:, None, :] - up_mean[:, None, None] - x_hat * proj_term)
    return grad_x.astype(jnp.bfloat16), grad_gamma, grad_beta


def head_rows(feat_rows, label_rows, ln_gamma, ln_beta, w_head, b_head):
    x_hat, inv_std, x_hat_mean, pooled16 = norm_pool(feat_rows, ln_gamma, ln_beta)
    col_ids = jnp.arange(PADDED_CLASSES)
    valid_mask = col_ids < CLASSES
    logits = jnp.dot(pooled16, w_head, preferred_element_type=jnp.float32) + b_head
    logits = jnp.where(valid_mask, logits, -1e30)
    row_max = jnp.max(logits, axis=-1, keepdims=True)
    log_norm = row_max + jnp.log(jnp.sum(jnp.exp(logits - row_max), axis=-1, keepdims=True))
    onehot = col_ids == label_rows[:, None]
    target = jnp.sum(jnp.where(onehot, logits, 0.0), axis=-1)
    valid_sum = jnp.sum(jnp.where(valid_mask, logits, 0.0), axis=-1)
    loss_rows = log_norm[:, 0] - (1.0 - SMOOTH) * target - (SMOOTH / CLASSES) * valid_sum
    soft_probs = jnp.exp(logits - log_norm)
    dlogit = (soft_probs - (1.0 - SMOOTH) * onehot - (SMOOTH / CLASSES) * valid_mask) / GLOBAL_BATCH
    dlogit16 = dlogit.astype(jnp.bfloat16)
    grad_w = jnp.dot(pooled16.T, dlogit16, preferred_element_type=jnp.float32)
    grad_b = jnp.sum(dlogit, axis=0)
    grad_pool = jnp.dot(dlogit16, w_head.T, preferred_element_type=jnp.float32)
    grad_x, grad_gamma, grad_beta = norm_backward(grad_pool, x_hat, inv_std, x_hat_mean, ln_gamma)
    return jnp.sum(loss_rows), grad_x, grad_w, grad_b, grad_gamma, grad_beta


def reference(feats, ln_gamma, ln_beta, w_head, b_head, labels):
    block_count = GLOBAL_BATCH // ROW_BLOCK
    feat_blocks = feats.reshape(block_count, ROW_BLOCK, TOKENS, WIDTH)
    label_blocks = labels.reshape(block_count, ROW_BLOCK)
    init_carry = (jnp.zeros((), jnp.float32), jnp.zeros((WIDTH, PADDED_CLASSES), jnp.float32), jnp.zeros((PADDED_CLASSES,), jnp.float32), jnp.zeros((WIDTH,), jnp.float32), jnp.zeros((WIDTH,), jnp.float32))

    def scan_step(acc_carry, block_in):
        loss_sum, grad_x, grad_w, grad_b, grad_gamma, grad_beta = head_rows(block_in[0], block_in[1], ln_gamma, ln_beta, w_head, b_head)
        new_carry = (acc_carry[0] + loss_sum, acc_carry[1] + grad_w, acc_carry[2] + grad_b, acc_carry[3] + grad_gamma, acc_carry[4] + grad_beta)
        return new_carry, grad_x

    final_carry, grad_blocks = lax.scan(scan_step, init_carry, (feat_blocks, label_blocks))
    grad_feats = grad_blocks.reshape(GLOBAL_BATCH, TOKENS, WIDTH)
    return (final_carry[0] / GLOBAL_BATCH, grad_feats, final_carry[1], final_carry[2], final_carry[3], final_carry[4])
```

```python
import functools

import jax
import jax.numpy as jnp
from jax import lax
from jax.experimental import pallas as pl
from jax.experimental.pallas import tpu as pltpu
from jax.sharding import PartitionSpec as P

VALID_CLASSES = 21841
LN_EPS = 1e-5
SMOOTH = 0.1
MESH = pl.DeviceIdType.MESH
F32 = jnp.float32
BF16 = jnp.bfloat16
LANES = 128
SIDES = {128: (4, 4, 4), 16: (2, 2, 2)}


def lane_ids(shape):
    return lax.broadcasted_iota(jnp.int32, shape, len(shape) - 1)


def head_kernel(
    sides, rows_total, f_ref, gam_ref, bet_ref, w_hbm, b_ref, lab_ref,
    loss_ref, dw_ref, db_ref, dg_ref, dbt_ref, dpool_ref, st_ref,
    fbuf, w, pf, p16, lg, dl16, dwbuf, dwrecv, xm, dpp, dpf, labs,
    ra, rb, ra2, rb2, ta, tb, sy, sz, gx, gc,
    f_sem, w_sem, x_send, x_recv, xl_send, xl_recv, g_send, g_recv, y_send, y_recv, z_send, z_recv,
    r_send, r_recv, d_send, d_recv, o_sem, q_send, q_recv,
):
    nx, ny, nz = sides
    npl = ny * nz
    tokens, ti, width = f_ref.shape
    cols = w.shape[1]
    half = ti // 2
    pb = half // npl
    ya, za = half // ny, half // nz
    tp, dp = lax.axis_index("tp"), lax.axis_index("dp")
    zi, yi = tp // ny, lax.rem(tp, ny)
    xi, ci = dp // 2, lax.rem(dp, 2)
    groups = ti // 8

    def dev(x=xi, y=yi, z=zi, c=ci):
        return {"tp": z * ny + y, "dp": x * 2 + c}

    xpeer = [(d, lax.rem(xi + d, nx)) for d in range(1, nx)]
    ypeer = [(d, lax.rem(yi + d, ny)) for d in range(1, ny)]
    zpeer = [(d, lax.rem(zi + d, nz)) for d in range(1, nz)]

    def remote(src, dst, ss, rs, who):
        return pltpu.make_async_remote_copy(src_ref=src, dst_ref=dst, send_sem=ss, recv_sem=rs, device_id=who, device_id_type=MESH)

    barrier = pltpu.get_barrier_semaphore()
    everyone = [dev(x=x) for _, x in xpeer] + [dev(y=y) for _, y in ypeer] + [dev(z=z) for _, z in zpeer] + [dev(c=1 - ci)]
    for who in everyone:
        pl.semaphore_signal(barrier, inc=1, device_id=who, device_id_type=MESH)

    ia, ib = zi * ny + yi, yi * nz + zi
    nslot = fbuf.shape[0]

    def arow(j):
        return pl.multiple_of(lax.rem(ia + j, npl) * pb, 8)

    def brow(j):
        return pl.multiple_of(half + lax.rem(ib + j, npl) * pb, 8)

    def fetch(j):
        slot = lax.rem(j, nslot)
        ca = pltpu.make_async_copy(f_ref.at[:, pl.ds(arow(j), pb), :], fbuf.at[slot, 0], f_sem.at[slot, 0])
        cb = pltpu.make_async_copy(f_ref.at[:, pl.ds(brow(j), pb), :], fbuf.at[slot, 1], f_sem.at[slot, 1])
        return ca, cb

    for j in range(nslot):
        for c in fetch(j):
            c.start()
    w_copy = pltpu.make_async_copy(w_hbm, w, w_sem)
    w_copy.start()
    labs[0] = lab_ref[...]
    st_ref[...] = jnp.zeros_like(st_ref)

    def norm_rows(slot, h, row0):
        x = fbuf[slot, h].astype(F32)
        mean = jnp.sum(x, axis=-1, keepdims=True) * (1.0 / width)
        cen = x - mean
        var = jnp.sum(cen * cen, axis=-1, keepdims=True) * (1.0 / width)
        inv = lax.rsqrt(var + LN_EPS)
        hat = jnp.sum(cen * inv, axis=0) * (1.0 / tokens)
        xm[pl.ds(row0, pb), :] = hat
        pf[0, pl.ds(row0, pb), :] = (hat * gam_ref[...] + bet_ref[...]).astype(BF16).astype(F32)
        blk = row0 // 8
        ids = lane_ids((tokens, 8, LANES))
        st_ref[...] = jnp.where(ids == blk, mean, jnp.where(ids == blk + 64, inv, st_ref[...]))

    def norm_chunk(j, prefetch):
        slot = lax.rem(j, nslot)
        for c in fetch(j):
            c.wait()

        def one(h, _):
            norm_rows(slot, h, pl.multiple_of(jnp.where(h == 0, arow(j), brow(j)), 8))
            return 0

        lax.fori_loop(0, 2, one, 0)
        if prefetch:
            for c in fetch(j + nslot):
                c.start()

    def norm_chunks(lo, hi):
        for a, b, pre in ((lo, min(hi, npl - nslot), True), (max(lo, npl - nslot), hi, False)):
            if b > a:
                lax.fori_loop(a, b, lambda j, _, pre=pre: (norm_chunk(j, pre), 0)[1], 0)

    sched = [1 * npl // 16, 5 * npl // 16, 10 * npl // 16]
    sched[0] = 1
    norm_chunks(0, 1)
    pl.semaphore_wait(barrier, len(everyone))

    own_a, own_b = pl.ds(arow(0), pb), pl.ds(brow(0), pb)
    xs = []
    for d, x in xpeer:
        for k, rows in enumerate((own_a, own_b)):
            xs.append(remote(pf.at[0, rows], pf.at[nx - d, rows], x_send.at[d - 1, k], x_recv.at[nx - d - 1, k], dev(x=x)))
        xs.append(remote(labs.at[0], labs.at[nx - d], xl_send.at[d - 1], xl_recv.at[nx - d - 1], dev(x=x)))
    for c in xs:
        c.start()
    norm_chunks(1, sched[1])
    for c in xs:
        c.wait()

    g1 = []
    for d, y in ypeer:
        g1.append(remote(pf.at[pl.ds(1, nx - 1), own_a], pf.at[pl.ds(1, nx - 1), own_a], g_send.at[0, d - 1], g_recv.at[0, ny - d - 1], dev(y=y)))
    for d, z in zpeer:
        g1.append(remote(pf.at[pl.ds(1, nx - 1), own_b], pf.at[pl.ds(1, nx - 1), own_b], g_send.at[1, d - 1], g_recv.at[1, nz - d - 1], dev(z=z)))
    for c in g1:
        c.start()
    norm_chunks(sched[1], sched[2])
    for c in g1:
        c.wait()
    blk_a = pl.ds(pl.multiple_of(zi * za, 8), za)
    blk_b = pl.ds(pl.multiple_of(half + yi * ya, 8), ya)
    g2 = []
    for d, z in zpeer:
        g2.append(remote(pf.at[pl.ds(1, nx - 1), blk_a], pf.at[pl.ds(1, nx - 1), blk_a], g_send.at[2, d - 1], g_recv.at[2, nz - d - 1], dev(z=z)))
    for d, y in ypeer:
        g2.append(remote(pf.at[pl.ds(1, nx - 1), blk_b], pf.at[pl.ds(1, nx - 1), blk_b], g_send.at[3, d - 1], g_recv.at[3, ny - d - 1], dev(y=y)))
    for c in g2:
        c.start()
    norm_chunks(sched[2], npl)
    w_copy.wait()

    col = (tp * cols + lane_ids((1, cols))).astype(F32)
    valid = col < float(VALID_CLASSES)
    vweight = jnp.where(valid, SMOOTH / VALID_CLASSES, 0.0)
    sub = 32
    lane8 = lane_ids((8, LANES))

    def col_of(packed, lane):
        return jnp.sum(jnp.where(lane8 == lane, packed, 0.0), axis=-1, keepdims=True)

    def label_col(slot, r):
        return jnp.concatenate([col_of(labs[slot], r * (sub // 8) + k) for k in range(sub // 8)], axis=0)

    sy[yi] = jnp.zeros_like(sy[0])

    def logits_of(slot):
        xabs = lax.rem(xi + slot, nx)
        p16[xabs] = pf[slot].astype(BF16)
        lg[xabs] = jnp.dot(p16[xabs], w[...], preferred_element_type=F32)

        def body(r, _):
            rows = pl.ds(pl.multiple_of(r * sub, sub), sub)
            l = jnp.where(valid, lg[xabs, rows, :] + b_ref[...], -1e30)
            m = jnp.max(l, axis=-1, keepdims=True)
            e = jnp.exp(l - m)
            s = jnp.sum(e, axis=-1, keepdims=True)
            lg[xabs, rows, :] = e
            hot = col == label_col(slot, r)
            part = jnp.where(hot, (1.0 - SMOOTH) * l, 0.0) + vweight * l
            ps = jnp.sum(part, axis=-1, keepdims=True)
            ms, ss, pp = sy[yi, 0], sy[yi, 1], sy[yi, 2]
            for k in range(sub // 8):
                here = lane8 == xabs * groups + r * (sub // 8) + k
                ms = jnp.where(here, m[8 * k : 8 * k + 8], ms)
                ss = jnp.where(here, s[8 * k : 8 * k + 8], ss)
                pp = jnp.where(here, ps[8 * k : 8 * k + 8], pp)
            sy[yi, 0], sy[yi, 1], sy[yi, 2] = ms, ss, pp
            return 0

        lax.fori_loop(0, ti // sub, body, 0)

    logits_of(0)
    for c in g2:
        c.wait()
    lax.fori_loop(1, nx, lambda s, _: (logits_of(s), 0)[1], 0)
    mine_m = sy[yi, 0]

    st1 = [remote(sy.at[yi], sy.at[yi], y_send.at[d - 1], y_recv.at[ny - d - 1], dev(y=y)) for d, y in ypeer]
    for c in st1:
        c.start()
    for c in st1:
        c.wait()

    def merge(buf, n):
        m = buf[0, 0]
        for k in range(1, n):
            m = jnp.maximum(m, buf[k, 0])
        s = jnp.zeros_like(m)
        q = jnp.zeros_like(m)
        for k in range(n):
            s = s + buf[k, 1] * jnp.exp(buf[k, 0] - m)
            q = q + buf[k, 2]
        return m, s, q

    m, s, q = merge(sy, ny)
    sz[zi, 0], sz[zi, 1], sz[zi, 2] = m, s, q
    st2 = [remote(sz.at[zi], sz.at[zi], z_send.at[d - 1], z_recv.at[nz - d - 1], dev(z=z)) for d, z in zpeer]
    for c in st2:
        c.start()
    for c in st2:
        c.wait()
    m, s, q = merge(sz, nz)
    used = lane8 < nx * groups
    coef = jnp.where(used, jnp.exp(mine_m - m) / s * (1.0 / rows_total), 0.0)
    loss_rows = jnp.where(used, m + jnp.log(jnp.where(used, s, 1.0)) - q, 0.0)
    sz[zi, 0] = coef
    vscaled = vweight * (1.0 / rows_total)
    hotscaled = (1.0 - SMOOTH) / rows_total

    def dlogit_of(slot, acc):
        xabs = lax.rem(xi + slot, nx)

        def body(r, acc):
            rows = pl.ds(pl.multiple_of(r * sub, sub), sub)
            cc = sz[zi, 0]
            cf = jnp.concatenate([col_of(cc, xabs * groups + r * (sub // 8) + k) for k in range(sub // 8)], axis=0)
            hot = col == label_col(slot, r)
            dl = lg[xabs, rows, :] * cf - jnp.where(hot, hotscaled, 0.0) - vscaled
            dl16[xabs, rows, :] = dl.astype(BF16)
            lg[xabs, rows, :] = dl
            return acc

        return lax.fori_loop(0, ti // sub, body, acc)

    dlogit_of(0, 0)
    dpp[...] = lax.dot_general(dl16[xi], w[...], (((1,), (1,)), ((), ())), preferred_element_type=F32)

    r1 = []
    for d, z in zpeer:
        r1.append(remote(dpp.at[pl.ds(pl.multiple_of(z * za, 8), za)], ra.at[nz - d - 1], r_send.at[0, d - 1], r_recv.at[0, nz - d - 1], dev(z=z)))
    for d, y in ypeer:
        r1.append(remote(dpp.at[pl.ds(pl.multiple_of(half + y * ya, 8), ya)], rb.at[ny - d - 1], r_send.at[1, d - 1], r_recv.at[1, ny - d - 1], dev(y=y)))
    for c in r1:
        c.start()
    lax.fori_loop(1, nx, lambda s, a: dlogit_of(s, a), 0)

    def dbody(r, acc):
        return acc + lg[r // groups, pl.ds(pl.multiple_of(lax.rem(r, groups) * 8, 8), 8), :]

    db8 = lax.fori_loop(0, nx * groups, dbody, jnp.zeros((8, cols), F32))
    db_mine = jnp.sum(db8, axis=0, keepdims=True)
    for c in r1:
        c.wait()

    def total(buf, own, n):
        t = own
        for k in range(n - 1):
            t = t + buf[k]
        return t

    ta[...] = total(ra, dpp[blk_a, :], nz)
    tb[...] = total(rb, dpp[blk_b, :], ny)
    r2 = []
    for d, y in ypeer:
        r2.append(remote(ta.at[pl.ds(pl.multiple_of(y * pb, 8), pb)], ra2.at[ny - d - 1], r_send.at[2, d - 1], r_recv.at[2, ny - d - 1], dev(y=y)))
    for d, z in zpeer:
        r2.append(remote(tb.at[pl.ds(pl.multiple_of(z * pb, 8), pb)], rb2.at[nz - d - 1], r_send.at[3, d - 1], r_recv.at[3, nz - d - 1], dev(z=z)))
    for c in r2:
        c.start()

    mh = width // 2

    def dw_half(h):
        lhs_cols = pl.ds(pl.multiple_of(h * mh, 128), mh)
        k = nx * ti
        dwbuf[h] = lax.dot_general(p16[:, :, lhs_cols].reshape(k, mh), dl16[...].reshape(k, cols), (((0,), (0,)), ((), ())), preferred_element_type=F32)

    dw_half(1 - ci)
    ex = remote(dwbuf.at[1 - ci], dwrecv, d_send.at[0], d_recv.at[0], dev(c=1 - ci))
    ex.start()
    for c in r2:
        c.wait()
    dpf[own_a, :] = total(ra2, ta[pl.ds(pl.multiple_of(yi * pb, 8), pb), :], ny)
    dpf[own_b, :] = total(rb2, tb[pl.ds(pl.multiple_of(zi * pb, 8), pb), :], nz)
    a1 = []
    for d, y in ypeer:
        a1.append(remote(dpf.at[own_a], dpf.at[own_a], r_send.at[4, d - 1], r_recv.at[4, ny - d - 1], dev(y=y)))
    for d, z in zpeer:
        a1.append(remote(dpf.at[own_b], dpf.at[own_b], r_send.at[5, d - 1], r_recv.at[5, nz - d - 1], dev(z=z)))
    for c in a1:
        c.start()
    dw_half(ci)
    for c in a1:
        c.wait()
    a2 = []
    for d, z in zpeer:
        a2.append(remote(dpf.at[blk_a], dpf.at[blk_a], r_send.at[6, d - 1], r_recv.at[6, nz - d - 1], dev(z=z)))
    for d, y in ypeer:
        a2.append(remote(dpf.at[blk_b], dpf.at[blk_b], r_send.at[7, d - 1], r_recv.at[7, ny - d - 1], dev(y=y)))
    for c in a2:
        c.start()
    ex.wait()
    dwbuf[ci] = dwbuf[ci] + dwrecv[...]
    out_rows = pl.ds(pl.multiple_of(ci * mh, 8), mh)
    o_local = pltpu.make_async_copy(dwbuf.at[ci], dw_ref.at[out_rows], o_sem)
    o_far = remote(dwbuf.at[ci], dw_ref.at[out_rows], d_send.at[1], d_recv.at[1], dev(c=1 - ci))
    o_local.start()
    o_far.start()
    for c in a2:
        c.wait()
    dpool_ref[...] = dpf[...]

    gx[xi, 0:1, :] = jnp.sum(dpf[...] * xm[...], axis=0, keepdims=True)
    gx[xi, 1:2, :] = jnp.sum(dpf[...], axis=0, keepdims=True)
    t1 = [remote(gx.at[xi], gx.at[xi], q_send.at[d - 1], q_recv.at[nx - d - 1], dev(x=x)) for d, x in xpeer]
    for c in t1:
        c.start()
    for c in t1:
        c.wait()
    tot = gx[0]
    for k in range(1, nx):
        tot = tot + gx[k]
    gc[0, :, 0:width] = tot
    gc[0, 0:1, width : width + cols] = db_mine
    gc[0, :, width + cols :] = loss_rows
    t2 = remote(gc.at[0], gc.at[1], q_send.at[nx - 1], q_recv.at[nx - 1], dev(c=1 - ci))
    t2.start()
    t2.wait()
    both = gc[0] + gc[1]
    dg_ref[...] = both[0:1, 0:width]
    dbt_ref[...] = both[1:2, 0:width]
    db_ref[...] = both[0:1, width : width + cols]
    lsum = jnp.sum(jnp.sum(both[:, width + cols :], axis=-1, keepdims=True), axis=0, keepdims=True)
    loss_ref[...] = jnp.broadcast_to(lsum * (1.0 / rows_total), loss_ref.shape)
    o_local.wait()
    o_far.wait()


def norm_bwd_kernel(blocks, f_ref, dp_ref, gam_ref, st_ref, out_ref):
    tokens, rows, width = f_ref.shape
    i = pl.program_id(0)
    ids = lane_ids((tokens, 8, LANES))

    def one(h, _):
        r = pl.ds(pl.multiple_of(h * 8, 8), 8)
        blk = i * (rows // 8) + h
        u = dp_ref[r, :] * gam_ref[...] * (1.0 / tokens)
        ut = u - jnp.mean(u, axis=-1, keepdims=True)
        st = st_ref[...]
        mean = jnp.sum(jnp.where(ids == blk, st, 0.0), axis=-1, keepdims=True)
        inv = jnp.sum(jnp.where(ids == blk + 64, st, 0.0), axis=-1, keepdims=True)
        cen = f_ref[:, r, :].astype(F32) - mean
        proj = jnp.sum(cen * ut[None], axis=-1, keepdims=True) * inv * (1.0 / width)
        out_ref[:, r, :] = (inv * (ut[None] - cen * (inv * proj))).astype(BF16)
        return 0

    lax.fori_loop(0, rows // 8, one, 0)


def solution(mesh):
    sides = SIDES[mesh.devices.size]
    nx, ny, nz = sides
    dp_size = mesh.shape["dp"]

    def local_head(feats, ln_gamma, ln_beta, w_head, b_head, labels):
        ti, tokens, width = feats.shape
        cols = w_head.shape[1]
        half = ti // 2
        pb = half // (ny * nz)
        ft = jnp.transpose(feats, (1, 0, 2))
        gam, bet, bias = ln_gamma[None], ln_beta[None], b_head[None]
        lab = jnp.pad(labels.astype(F32).reshape(ti // 8, 8).T, ((0, 0), (0, LANES - ti // 8)))
        vm = pl.BlockSpec(memory_space=pltpu.VMEM)
        hbm = pl.BlockSpec(memory_space=pl.ANY)
        sem = pltpu.SemaphoreType.DMA
        n3 = max(nx, ny, nz)
        S = jax.ShapeDtypeStruct
        loss, dw, db, dg, dbt, dpool, st = pl.pallas_call(
            functools.partial(head_kernel, sides, ti * dp_size),
            out_shape=(S((8, LANES), F32), S((width, cols), F32), S((1, cols), F32), S((1, width), F32), S((1, width), F32), S((ti, width), F32), S((tokens, 8, LANES), F32)),
            in_specs=[hbm, vm, vm, hbm, vm, vm],
            out_specs=(vm, hbm, vm, vm, vm, vm, vm),
            scratch_shapes=[
                pltpu.VMEM((min(4, ny * nz), 2, tokens, pb, width), BF16),
                pltpu.VMEM((width, cols), BF16),
                pltpu.VMEM((nx, ti, width), F32),
                pltpu.VMEM((nx, ti, width), BF16),
                pltpu.VMEM((nx, ti, cols), F32),
                pltpu.VMEM((nx, ti, cols), BF16),
                pltpu.VMEM((2, width // 2, cols), F32),
                pltpu.VMEM((width // 2, cols), F32),
                pltpu.VMEM((ti, width), F32),
                pltpu.VMEM((ti, width), F32),
                pltpu.VMEM((ti, width), F32),
                pltpu.VMEM((nx, 8, LANES), F32),
                pltpu.VMEM((nz - 1, half // nz, width), F32),
                pltpu.VMEM((ny - 1, half // ny, width), F32),
                pltpu.VMEM((ny - 1, pb, width), F32),
                pltpu.VMEM((nz - 1, pb, width), F32),
                pltpu.VMEM((half // nz, width), F32),
                pltpu.VMEM((half // ny, width), F32),
                pltpu.VMEM((ny, 3, 8, LANES), F32),
                pltpu.VMEM((nz, 3, 8, LANES), F32),
                pltpu.VMEM((nx, 8, width), F32),
                pltpu.VMEM((2, 8, width + cols + LANES), F32),
                sem((min(4, ny * nz), 2)),
                sem,
                sem((nx - 1, 2)), sem((nx - 1, 2)), sem((nx - 1,)), sem((nx - 1,)),
                sem((4, n3 - 1)), sem((4, n3 - 1)),
                sem((ny - 1,)), sem((ny - 1,)), sem((nz - 1,)), sem((nz - 1,)),
                sem((8, n3 - 1)), sem((8, n3 - 1)),
                sem((2,)), sem((2,)), sem,
                sem((nx,)), sem((nx,)),
            ],
            compiler_params=pltpu.CompilerParams(collective_id=0, has_side_effects=True, vmem_limit_bytes=60 * 1024 * 1024),
        )(ft, gam, bet, w_head, bias, lab)
        rb = 16
        dft = pl.pallas_call(
            functools.partial(norm_bwd_kernel, ti // 8),
            grid=(ti // rb,),
            out_shape=S((tokens, ti, width), BF16),
            in_specs=[
                pl.BlockSpec((tokens, rb, width), lambda i: (0, i, 0)),
                pl.BlockSpec((rb, width), lambda i: (i, 0)),
                pl.BlockSpec((1, width), lambda i: (0, 0)),
                pl.BlockSpec((tokens, 8, LANES), lambda i: (0, 0, 0)),
            ],
            out_specs=pl.BlockSpec((tokens, rb, width), lambda i: (0, i, 0)),
            compiler_params=pltpu.CompilerParams(vmem_limit_bytes=40 * 1024 * 1024),
        )(ft, dpool, gam, st)
        return loss[0, 0], jnp.transpose(dft, (1, 0, 2)), dw, db[0], dg[0], dbt[0]

    return jax.shard_map(
        local_head,
        mesh=mesh,
        in_specs=(P("dp", None, None), P(), P(), P(None, "tp"), P("tp"), P("dp")),
        out_specs=(P(), P("dp", None, None), P(None, "tp"), P("tp"), P(), P()),
        check_vma=False,
    )
```

```python
import functools

import jax
import jax.numpy as jnp
from jax import lax
from jax.experimental import pallas as pl
from jax.experimental.pallas import tpu as pltpu
from jax.sharding import PartitionSpec as P

VALID_CLASSES = 21841
LN_EPS = 1e-5
SMOOTH = 0.1
MESH = pl.DeviceIdType.MESH
F32 = jnp.float32
BF16 = jnp.bfloat16
LANES = 128
SIDES = {128: (4, 4, 4), 16: (2, 2, 2)}


def lane_ids(shape):
    return lax.broadcasted_iota(jnp.int32, shape, len(shape) - 1)


def head_kernel(
    sides, rows_total, f_ref, gam_ref, bet_ref, w_hbm, b_ref, lab_ref,
    dwbuf, small_ref, dpf, st_ref,
    fbuf, w, pf, p16, lg, dl16, dwpart, dwrecv, xm, dpp, labs,
    ra, rb, ra2, rb2, ta, tb, stat, cof, gy, gz, gx, gc,
    f_sem, w_sem, x_send, x_recv, xl_send, xl_recv, xd_send, xd_recv, g_send, g_recv, s_send, s_recv,
    r_send, r_recv, d_send, d_recv, q_send, q_recv,
):
    nx, ny, nz = sides
    npl = ny * nz
    tokens, ti, width = f_ref.shape
    cols = w.shape[1]
    direct = width * 3 // 8
    half = ti // 2
    pb = half // npl
    ya, za = half // ny, half // nz
    tp, dp = lax.axis_index("tp"), lax.axis_index("dp")
    zi, yi = tp // ny, lax.rem(tp, ny)
    xi, ci = dp // 2, lax.rem(dp, 2)
    groups = ti // 8

    def dev(x=xi, y=yi, z=zi, c=ci):
        return {"tp": z * ny + y, "dp": x * 2 + c}

    xpeer = [(d, lax.rem(xi + d, nx)) for d in range(1, nx)]
    ypeer = [(d, lax.rem(yi + d, ny)) for d in range(1, ny)]
    zpeer = [(d, lax.rem(zi + d, nz)) for d in range(1, nz)]

    def remote(src, dst, ss, rs, who):
        return pltpu.make_async_remote_copy(src_ref=src, dst_ref=dst, send_sem=ss, recv_sem=rs, device_id=who, device_id_type=MESH)

    barrier = pltpu.get_barrier_semaphore()
    plane = [(dz * ny + dy, dev(y=lax.rem(yi + dy, ny), z=lax.rem(zi + dz, nz))) for dz in range(nz) for dy in range(ny) if dz or dy]
    everyone = [dev(x=x) for _, x in xpeer] + [who for _, who in plane] + [dev(c=1 - ci)]
    for who in everyone:
        pl.semaphore_signal(barrier, inc=1, device_id=who, device_id_type=MESH)

    ia, ib = zi * ny + yi, yi * nz + zi
    nslot = fbuf.shape[0]

    def arow(j):
        return pl.multiple_of(lax.rem(ia + j, npl) * pb, 8)

    def brow(j):
        return pl.multiple_of(half + lax.rem(ib + j, npl) * pb, 8)

    def fetch(j):
        slot = lax.rem(j, nslot)
        ca = pltpu.make_async_copy(f_ref.at[:, pl.ds(arow(j), pb), :], fbuf.at[slot, 0], f_sem.at[slot, 0])
        cb = pltpu.make_async_copy(f_ref.at[:, pl.ds(brow(j), pb), :], fbuf.at[slot, 1], f_sem.at[slot, 1])
        return ca, cb

    for j in range(nslot):
        for c in fetch(j):
            c.start()
    w_copy = pltpu.make_async_copy(w_hbm, w, w_sem)
    w_copy.start()
    st_ref[...] = jnp.zeros_like(st_ref)
    lane8 = lane_ids((8, LANES))
    row8 = lax.broadcasted_iota(jnp.int32, (8, LANES), 0)

    def norm_rows(slot, h, row0):
        x = fbuf[slot, h].astype(F32)
        mean = jnp.sum(x, axis=-1, keepdims=True) * (1.0 / width)
        cen = x - mean
        var = jnp.sum(cen * cen, axis=-1, keepdims=True) * (1.0 / width)
        inv = lax.rsqrt(var + LN_EPS)
        hat = jnp.sum(cen * inv, axis=0) * (1.0 / tokens)
        xm[pl.ds(row0, pb), :] = hat
        pf[0, pl.ds(row0, pb), :] = (hat * gam_ref[...] + bet_ref[...]).astype(BF16).astype(F32)
        blk = row0 // 8
        ids = lane_ids((tokens, 8, LANES))
        st_ref[...] = jnp.where(ids == blk, mean, jnp.where(ids == blk + 64, inv, st_ref[...]))

    def norm_chunk(j, prefetch):
        slot = lax.rem(j, nslot)
        for c in fetch(j):
            c.wait()

        def one(h, _):
            norm_rows(slot, h, pl.multiple_of(jnp.where(h == 0, arow(j), brow(j)), 8))
            return 0

        lax.fori_loop(0, 2, one, 0)
        if prefetch:
            for c in fetch(j + nslot):
                c.start()

    def norm_chunks(lo, hi):
        for a, b, pre in ((lo, min(hi, npl - nslot), True), (max(lo, npl - nslot), hi, False)):
            if b > a:
                lax.fori_loop(a, b, lambda j, _, pre=pre: (norm_chunk(j, pre), 0)[1], 0)

    dcols, pcols = pl.ds(0, direct), pl.ds(direct, width - direct)

    def straight(j):
        out = []
        for d, x in xpeer:
            for rows in (arow(j), brow(j)):
                rows = pl.ds(rows, pb)
                out.append(remote(pf.at[0, rows, dcols], pf.at[nx - d, rows, dcols], xd_send.at[d - 1], xd_recv.at[nx - d - 1], dev(x=x)))
        return out

    def send_straight(j):
        for c in straight(j):
            c.start()

    def norm_and_send(lo, hi):
        for a, b, pre in ((lo, min(hi, npl - nslot), True), (max(lo, npl - nslot), hi, False)):
            if b > a:
                lax.fori_loop(a, b, lambda j, _, pre=pre: (norm_chunk(j, pre), send_straight(j), 0)[2], 0)

    first = min(3, npl // 2)
    cuts = [first, npl // 2, npl * 13 // 16]
    norm_chunks(0, first)

    def pack_labels(g, acc):
        for k in range(8):
            acc = jnp.where((lane8 == g) & (row8 == k), lab_ref[g * 8 + k].astype(F32), acc)
        return acc

    labs[0] = lax.fori_loop(0, groups, pack_labels, jnp.zeros((8, LANES), F32))
    pl.semaphore_wait(barrier, len(everyone))

    own_a, own_b = pl.ds(arow(0), pb), pl.ds(brow(0), pb)
    order = sorted(range(1, nx), key=lambda slot: min(slot, nx - slot))
    xs = {}
    for d, x in sorted(xpeer, key=lambda dx: min(dx[0], nx - dx[0])):
        xs[nx - d] = []
        for k, rows in enumerate((own_a, own_b)):
            xs[nx - d].append(remote(pf.at[0, rows, pcols], pf.at[nx - d, rows, pcols], x_send.at[nx - d - 1, k], x_recv.at[nx - d - 1, k], dev(x=x)))
        xs[nx - d].append(remote(labs.at[0], labs.at[nx - d], xl_send.at[nx - d - 1], xl_recv.at[nx - d - 1], dev(x=x)))
        for c in xs[nx - d]:
            c.start()
    lax.fori_loop(0, first, lambda j, _: (send_straight(j), 0)[1], 0)
    norm_and_send(first, cuts[1])

    blk_a = pl.ds(pl.multiple_of(zi * za, 8), za)
    blk_b = pl.ds(pl.multiple_of(half + yi * ya, 8), ya)
    g1, g2 = {}, {}
    for slot in order:
        for c in xs[slot]:
            c.wait()
        g1[slot] = []
        for k, peers, n, rows in ((0, [(d, dev(y=y)) for d, y in ypeer], ny, own_a), (1, [(d, dev(z=z)) for d, z in zpeer], nz, own_b)):
            for d, who in peers:
                ref = pf.at[slot, rows, pcols]
                g1[slot].append(remote(ref, ref, g_send.at[k, slot - 1, d - 1], g_recv.at[k, slot - 1, n - d - 1], who))
        for c in g1[slot]:
            c.start()
    norm_and_send(cuts[1], cuts[2])
    for slot in order:
        for c in g1[slot]:
            c.wait()
        g2[slot] = []
        for k, peers, n, rows in ((2, [(d, dev(z=z)) for d, z in zpeer], nz, blk_a), (3, [(d, dev(y=y)) for d, y in ypeer], ny, blk_b)):
            for d, who in peers:
                ref = pf.at[slot, rows, pcols]
                g2[slot].append(remote(ref, ref, g_send.at[k, slot - 1, d - 1], g_recv.at[k, slot - 1, n - d - 1], who))
        for c in g2[slot]:
            c.start()
    norm_and_send(cuts[2], npl)
    w_copy.wait()

    col = (tp * cols + lane_ids((1, cols))).astype(F32)
    valid = col < float(VALID_CLASSES)
    vweight = jnp.where(valid, SMOOTH / VALID_CLASSES, 0.0)
    sub = 32

    def col_of(packed, lane):
        return jnp.sum(jnp.where(lane8 == lane, packed, 0.0), axis=-1, keepdims=True)

    def label_col(slot, r):
        return jnp.concatenate([col_of(labs[slot], r * (sub // 8) + k) for k in range(sub // 8)], axis=0)

    stat[tp] = jnp.zeros_like(stat[0])
    bias = b_ref[...].reshape(1, cols)

    def logits_of(slot):
        xabs = lax.rem(xi + slot, nx)
        p16[xabs] = pf[slot].astype(BF16)
        lg[xabs] = jnp.dot(p16[xabs], w[...], preferred_element_type=F32)

        def body(r, _):
            rows = pl.ds(pl.multiple_of(r * sub, sub), sub)
            l = jnp.where(valid, lg[xabs, rows, :] + bias, -1e30)
            m = jnp.max(l, axis=-1, keepdims=True)
            e = jnp.exp(l - m)
            s = jnp.sum(e, axis=-1, keepdims=True)
            lg[xabs, rows, :] = e
            hot = col == label_col(slot, r)
            part = jnp.where(hot, (1.0 - SMOOTH) * l, 0.0) + vweight * l
            ps = jnp.sum(part, axis=-1, keepdims=True)
            ms, ss, pp = stat[tp, 0], stat[tp, 1], stat[tp, 2]
            for k in range(sub // 8):
                here = lane8 == xabs * groups + r * (sub // 8) + k
                ms = jnp.where(here, m[8 * k : 8 * k + 8], ms)
                ss = jnp.where(here, s[8 * k : 8 * k + 8], ss)
                pp = jnp.where(here, ps[8 * k : 8 * k + 8], pp)
            stat[tp, 0], stat[tp, 1], stat[tp, 2] = ms, ss, pp
            return 0

        lax.fori_loop(0, ti // sub, body, 0)

    logits_of(0)
    for slot in order:
        for c in g2[slot]:
            c.wait()
        ref = pf.at[slot, :, dcols]
        whole = remote(ref, ref, xd_send.at[nx - slot - 1], xd_recv.at[slot - 1], dev(x=xpeer[slot - 1][1]))
        whole.wait_recv()
        logits_of(slot)
    mine_m = stat[tp, 0]

    st1 = [remote(stat.at[tp], stat.at[tp], s_send.at[k - 1], s_recv.at[k - 1], who) for k, who in plane]
    for c in st1:
        c.start()
    for slot in order:
        ref = pf.at[slot, :, dcols]
        remote(ref, ref, xd_send.at[slot - 1], xd_recv.at[slot - 1], dev(x=xpeer[slot - 1][1])).wait_send()
    for c in st1:
        c.wait()
    m = stat[0, 0]
    for k in range(1, npl):
        m = jnp.maximum(m, stat[k, 0])
    s = jnp.zeros_like(m)
    q = jnp.zeros_like(m)
    for k in range(npl):
        s = s + stat[k, 1] * jnp.exp(stat[k, 0] - m)
        q = q + stat[k, 2]
    used = lane8 < nx * groups
    coef = jnp.where(used, jnp.exp(mine_m - m) / s * (1.0 / rows_total), 0.0)
    loss_rows = jnp.where(used, m + jnp.log(jnp.where(used, s, 1.0)) - q, 0.0)
    cof[...] = coef
    vscaled = vweight * (1.0 / rows_total)
    hotscaled = (1.0 - SMOOTH) / rows_total

    def dlogit_of(slot, acc):
        xabs = lax.rem(xi + slot, nx)

        def body(r, acc):
            rows = pl.ds(pl.multiple_of(r * sub, sub), sub)
            cc = cof[...]
            cf = jnp.concatenate([col_of(cc, xabs * groups + r * (sub // 8) + k) for k in range(sub // 8)], axis=0)
            hot = col == label_col(slot, r)
            dl = lg[xabs, rows, :] * cf - jnp.where(hot, hotscaled, 0.0) - vscaled
            dl16[xabs, rows, :] = dl.astype(BF16)
            lg[xabs, rows, :] = dl
            return acc

        return lax.fori_loop(0, ti // sub, body, acc)

    dlogit_of(0, 0)
    dpp[...] = lax.dot_general(dl16[xi], w[...], (((1,), (1,)), ((), ())), preferred_element_type=F32)

    r1 = []
    for d, z in zpeer:
        r1.append(remote(dpp.at[pl.ds(pl.multiple_of(z * za, 8), za)], ra.at[nz - d - 1], r_send.at[0, d - 1], r_recv.at[0, nz - d - 1], dev(z=z)))
    for d, y in ypeer:
        r1.append(remote(dpp.at[pl.ds(pl.multiple_of(half + y * ya, 8), ya)], rb.at[ny - d - 1], r_send.at[1, d - 1], r_recv.at[1, ny - d - 1], dev(y=y)))
    for c in r1:
        c.start()
    lax.fori_loop(1, nx, lambda s, a: dlogit_of(s, a), 0)

    for c in r1:
        c.wait()

    def total(buf, own, n):
        t = own
        for k in range(n - 1):
            t = t + buf[k]
        return t

    ta[...] = total(ra, dpp[blk_a, :], nz)
    tb[...] = total(rb, dpp[blk_b, :], ny)
    r2 = []
    for d, y in ypeer:
        r2.append(remote(ta.at[pl.ds(pl.multiple_of(y * pb, 8), pb)], ra2.at[ny - d - 1], r_send.at[2, d - 1], r_recv.at[2, ny - d - 1], dev(y=y)))
    for d, z in zpeer:
        r2.append(remote(tb.at[pl.ds(pl.multiple_of(z * pb, 8), pb)], rb2.at[nz - d - 1], r_send.at[3, d - 1], r_recv.at[3, nz - d - 1], dev(z=z)))
    for c in r2:
        c.start()

    mh = width // 2

    def dw_half(h, out):
        lhs_cols = pl.ds(pl.multiple_of(h * mh, 128), mh)
        k = nx * ti
        out[...] = lax.dot_general(p16[:, :, lhs_cols].reshape(k, mh), dl16[...].reshape(k, cols), (((0,), (0,)), ((), ())), preferred_element_type=F32)

    dw_half(1 - ci, dwpart)
    ex = remote(dwpart, dwrecv, d_send.at[0], d_recv.at[0], dev(c=1 - ci))
    ex.start()
    for c in r2:
        c.wait()
    dpf[own_a, :] = total(ra2, ta[pl.ds(pl.multiple_of(yi * pb, 8), pb), :], ny)
    dpf[own_b, :] = total(rb2, tb[pl.ds(pl.multiple_of(zi * pb, 8), pb), :], nz)
    gy[yi, 0:1, :] = jnp.sum(dpf[own_a, :] * xm[own_a, :] + dpf[own_b, :] * xm[own_b, :], axis=0, keepdims=True)
    gy[yi, 1:2, :] = jnp.sum(dpf[own_a, :] + dpf[own_b, :], axis=0, keepdims=True)
    a1 = []
    for d, y in ypeer:
        a1.append(remote(dpf.at[own_a], dpf.at[own_a], r_send.at[4, d - 1], r_recv.at[4, ny - d - 1], dev(y=y)))
    for d, z in zpeer:
        a1.append(remote(dpf.at[own_b], dpf.at[own_b], r_send.at[5, d - 1], r_recv.at[5, nz - d - 1], dev(z=z)))
    for d, y in ypeer:
        a1.append(remote(gy.at[yi], gy.at[yi], q_send.at[0, d - 1], q_recv.at[0, ny - d - 1], dev(y=y)))
    for c in a1:
        c.start()
    dw_half(ci, dwbuf.at[0])

    def dbody(r, acc):
        return acc + lg[r // groups, pl.ds(pl.multiple_of(lax.rem(r, groups) * 8, 8), 8), :]

    db8 = lax.fori_loop(0, nx * groups, dbody, jnp.zeros((8, cols), F32))
    for c in a1:
        c.wait()
    a2 = []
    for d, z in zpeer:
        a2.append(remote(dpf.at[blk_a], dpf.at[blk_a], r_send.at[6, d - 1], r_recv.at[6, nz - d - 1], dev(z=z)))
    for d, y in ypeer:
        a2.append(remote(dpf.at[blk_b], dpf.at[blk_b], r_send.at[7, d - 1], r_recv.at[7, ny - d - 1], dev(y=y)))

    def summed(buf, n):
        t = buf[0]
        for k in range(1, n):
            t = t + buf[k]
        return t

    gz[zi] = summed(gy, ny)
    t1 = [remote(gz.at[zi], gz.at[zi], q_send.at[1, d - 1], q_recv.at[1, nz - d - 1], dev(z=z)) for d, z in zpeer]
    for c in t1 + a2:
        c.start()
    ex.wait()
    dwbuf[0] = dwbuf[0] + dwrecv[...]
    back = remote(dwbuf.at[0], dwbuf.at[1], d_send.at[1], d_recv.at[1], dev(c=1 - ci))
    back.start()
    for c in t1:
        c.wait()
    gx[xi] = summed(gz, nz)
    t2 = [remote(gx.at[xi], gx.at[xi], q_send.at[2, d - 1], q_recv.at[2, nx - d - 1], dev(x=x)) for d, x in xpeer]
    for c in t2:
        c.start()
    gc[0] = jnp.zeros_like(gc[0])
    gc[0, 0:1, width : width + cols] = jnp.sum(db8, axis=0, keepdims=True)
    gc[0, :, width + cols :] = loss_rows
    for c in t2:
        c.wait()
    gc[0, :, 0:width] = summed(gx, nx)
    t3 = remote(gc.at[0], gc.at[1], q_send.at[3, 0], q_recv.at[3, 0], dev(c=1 - ci))
    t3.start()
    for c in a2:
        c.wait()
    t3.wait()
    small_ref[...] = gc[0] + gc[1]
    back.wait()


def norm_bwd_kernel(rows_total, f_ref, dp_ref, gam_ref, st_ref, dwin_ref, small_ref, out_ref, dw_ref, loss_ref, db_ref, dg_ref, dbt_ref):
    tokens, rows, width = f_ref.shape
    cols = db_ref.shape[0]
    i = pl.program_id(0)
    ids = lane_ids((tokens, 8, LANES))

    def one(h, _):
        r = pl.ds(pl.multiple_of(h * 8, 8), 8)
        blk = i * (rows // 8) + h
        u = dp_ref[r, :] * gam_ref[...] * (1.0 / tokens)
        ut = u - jnp.mean(u, axis=-1, keepdims=True)
        st = st_ref[...]
        mean = jnp.sum(jnp.where(ids == blk, st, 0.0), axis=-1, keepdims=True)
        inv = jnp.sum(jnp.where(ids == blk + 64, st, 0.0), axis=-1, keepdims=True)
        cen = f_ref[:, r, :].astype(F32) - mean
        proj = jnp.sum(cen * ut[None], axis=-1, keepdims=True) * inv * (1.0 / width)
        out_ref[:, r, :] = (inv * (ut[None] - cen * (inv * proj))).astype(BF16)
        return 0

    lax.fori_loop(0, rows // 8, one, 0)
    dr = dw_ref.shape[0]
    per = width // 2 // dr
    own = (i // per) == lax.rem(lax.axis_index("dp"), 2)
    dw_ref[...] = dwin_ref[jnp.where(own, 0, 1), pl.ds(pl.multiple_of(lax.rem(i, per) * dr, 8), dr), :]

    @pl.when(i == 0)
    def _():
        dg_ref[...] = small_ref[0:1, 0:width].reshape(width)
        dbt_ref[...] = small_ref[1:2, 0:width].reshape(width)
        db_ref[...] = small_ref[0:1, width : width + cols].reshape(cols)
        tail = jnp.sum(jnp.sum(small_ref[:, width + cols :], axis=-1, keepdims=True), axis=0, keepdims=True)
        loss_ref[...] = tail * (1.0 / rows_total)


def solution(mesh):
    sides = SIDES[mesh.devices.size]
    nx, ny, nz = sides
    dp_size = mesh.shape["dp"]

    def local_head(feats, ln_gamma, ln_beta, w_head, b_head, labels):
        ti, tokens, width = feats.shape
        cols = w_head.shape[1]
        half = ti // 2
        pb = half // (ny * nz)
        ft = jnp.transpose(feats, (1, 0, 2))
        gam, bet = ln_gamma[None], ln_beta[None]
        vm = pl.BlockSpec(memory_space=pltpu.VMEM)
        hbm = pl.BlockSpec(memory_space=pl.ANY)
        sm = pl.BlockSpec(memory_space=pltpu.SMEM)
        sem = pltpu.SemaphoreType.DMA
        n3 = max(nx, ny, nz)
        npl = ny * nz
        S = jax.ShapeDtypeStruct
        extra = width + cols + LANES
        dw, small, dpool, st = pl.pallas_call(
            functools.partial(head_kernel, sides, ti * dp_size),
            out_shape=(pltpu.VMEM((2, width // 2, cols), F32), pltpu.VMEM((8, extra), F32), pltpu.VMEM((ti, width), F32), pltpu.VMEM((tokens, 8, LANES), F32)),
            in_specs=[hbm, vm, vm, hbm, vm, sm],
            out_specs=(vm, vm, vm, vm),
            scratch_shapes=[
                pltpu.VMEM((min(4, npl), 2, tokens, pb, width), BF16),
                pltpu.VMEM((width, cols), BF16),
                pltpu.VMEM((nx, ti, width), F32),
                pltpu.VMEM((nx, ti, width), BF16),
                pltpu.VMEM((nx, ti, cols), F32),
                pltpu.VMEM((nx, ti, cols), BF16),
                pltpu.VMEM((width // 2, cols), F32),
                pltpu.VMEM((width // 2, cols), F32),
                pltpu.VMEM((ti, width), F32),
                pltpu.VMEM((ti, width), F32),
                pltpu.VMEM((nx, 8, LANES), F32),
                pltpu.VMEM((nz - 1, half // nz, width), F32),
                pltpu.VMEM((ny - 1, half // ny, width), F32),
                pltpu.VMEM((ny - 1, pb, width), F32),
                pltpu.VMEM((nz - 1, pb, width), F32),
                pltpu.VMEM((half // nz, width), F32),
                pltpu.VMEM((half // ny, width), F32),
                pltpu.VMEM((npl, 3, 8, LANES), F32),
                pltpu.VMEM((8, LANES), F32),
                pltpu.VMEM((ny, 8, width), F32),
                pltpu.VMEM((nz, 8, width), F32),
                pltpu.VMEM((nx, 8, width), F32),
                pltpu.VMEM((2, 8, extra), F32),
                sem((min(4, npl), 2)),
                sem,
                sem((nx - 1, 2)), sem((nx - 1, 2)), sem((nx - 1,)), sem((nx - 1,)), sem((nx - 1,)), sem((nx - 1,)),
                sem((4, nx - 1, n3 - 1)), sem((4, nx - 1, n3 - 1)),
                sem((npl - 1,)), sem((npl - 1,)),
                sem((8, n3 - 1)), sem((8, n3 - 1)),
                sem((2,)), sem((2,)),
                sem((4, n3 - 1)), sem((4, n3 - 1)),
            ],
            compiler_params=pltpu.CompilerParams(collective_id=0, has_side_effects=True, vmem_limit_bytes=48 * 1024 * 1024),
        )(ft, gam, bet, w_head, b_head, labels)
        rb = 16
        steps = ti // rb
        near = lambda a: pltpu.with_memory_space_constraint(a, pltpu.VMEM)
        dft, dwo, loss, db, dg, dbt = pl.pallas_call(
            functools.partial(norm_bwd_kernel, ti * dp_size),
            grid=(steps,),
            out_shape=(S((tokens, ti, width), BF16), S((width, cols), F32), S((1, 1), F32), S((cols,), F32), S((width,), F32), S((width,), F32)),
            in_specs=[
                pl.BlockSpec((tokens, rb, width), lambda i: (0, i, 0)),
                pl.BlockSpec((rb, width), lambda i: (i, 0)),
                pl.BlockSpec((1, width), lambda i: (0, 0)),
                vm, vm, vm,
            ],
            out_specs=(
                pl.BlockSpec((tokens, rb, width), lambda i: (0, i, 0)),
                pl.BlockSpec((width // steps, cols), lambda i: (i, 0)),
                vm, vm, vm, vm,
            ),
            compiler_params=pltpu.CompilerParams(vmem_limit_bytes=40 * 1024 * 1024),
        )(ft, dpool, gam, near(st), near(dw), near(small))
        return loss[0, 0], jnp.transpose(dft, (1, 0, 2)), dwo, db, dg, dbt

    return jax.shard_map(
        local_head,
        mesh=mesh,
        in_specs=(P("dp", None, None), P(), P(), P(None, "tp"), P("tp"), P("dp")),
        out_specs=(P(), P("dp", None, None), P(None, "tp"), P("tp"), P(), P()),
        check_vma=False,
    )
```

```python
import functools

import jax
import jax.numpy as jnp
from jax import lax
from jax.experimental import pallas as pl
from jax.experimental.pallas import tpu as pltpu
from jax.sharding import PartitionSpec as P

VALID_CLASSES = 21841
LN_EPS = 1e-5
SMOOTH = 0.1
MESH = pl.DeviceIdType.MESH
F32 = jnp.float32
BF16 = jnp.bfloat16
LANES = 128
SIDES = {128: (4, 4, 4), 16: (2, 2, 2)}


def lane_ids(shape):
    return lax.broadcasted_iota(jnp.int32, shape, len(shape) - 1)


def head_kernel(
    sides, rows_total, f_ref, gam_ref, bet_ref, w_hbm, b_ref, lab_ref,
    dwbuf, small_ref, dpf, st_ref,
    fbuf, w, pf, p16, lt, lg, dl16, dwpart, dwrecv, xm, dpp, labs,
    ra, rb, ra2, rb2, ta, tb, near, stat, cof, dbs, gy, gz, gx, gc,
    f_sem, w_sem, x_send, x_recv, xl_send, xl_recv, xd_send, xd_recv, g_send, g_recv, n_send, n_recv, s_send, s_recv,
    r_send, r_recv, d_send, d_recv, q_send, q_recv,
):
    nx, ny, nz = sides
    npl = ny * nz
    tokens, ti, width = f_ref.shape
    cols = w.shape[1]
    direct = width * 3 // 8
    half = ti // 2
    pb = half // npl
    ya, za = half // ny, half // nz
    tp, dp = lax.axis_index("tp"), lax.axis_index("dp")
    zi, yi = tp // ny, lax.rem(tp, ny)
    xi, ci = dp // 2, lax.rem(dp, 2)
    groups = ti // 8

    def dev(x=xi, y=yi, z=zi, c=ci):
        return {"tp": z * ny + y, "dp": x * 2 + c}

    xpeer = [(d, lax.rem(xi + d, nx)) for d in range(1, nx)]
    ypeer = [(d, lax.rem(yi + d, ny)) for d in range(1, ny)]
    zpeer = [(d, lax.rem(zi + d, nz)) for d in range(1, nz)]

    def remote(src, dst, ss, rs, who):
        return pltpu.make_async_remote_copy(src_ref=src, dst_ref=dst, send_sem=ss, recv_sem=rs, device_id=who, device_id_type=MESH)

    barrier = pltpu.get_barrier_semaphore()
    plane = [(dz * ny + dy, dev(y=lax.rem(yi + dy, ny), z=lax.rem(zi + dz, nz))) for dz in range(nz) for dy in range(ny) if dz or dy]
    everyone = [dev(x=x) for _, x in xpeer] + [who for _, who in plane] + [dev(c=1 - ci)]
    for who in everyone:
        pl.semaphore_signal(barrier, inc=1, device_id=who, device_id_type=MESH)

    ia, ib = zi * ny + yi, yi * nz + zi
    nslot = fbuf.shape[0]

    def arow(j):
        return pl.multiple_of(lax.rem(ia + j, npl) * pb, 8)

    def brow(j):
        return pl.multiple_of(half + lax.rem(ib + j, npl) * pb, 8)

    def fetch(j):
        slot = lax.rem(j, nslot)
        ca = pltpu.make_async_copy(f_ref.at[:, pl.ds(arow(j), pb), :], fbuf.at[slot, 0], f_sem.at[slot, 0])
        cb = pltpu.make_async_copy(f_ref.at[:, pl.ds(brow(j), pb), :], fbuf.at[slot, 1], f_sem.at[slot, 1])
        return ca, cb

    for j in range(nslot):
        for c in fetch(j):
            c.start()
    w_copy = pltpu.make_async_copy(w_hbm, w, w_sem)
    w_copy.start()
    st_ref[...] = jnp.zeros_like(st_ref)
    lane8 = lane_ids((8, LANES))
    row8 = lax.broadcasted_iota(jnp.int32, (8, LANES), 0)

    def norm_rows(slot, h, row0):
        x = fbuf[slot, h].astype(F32)
        mean = jnp.sum(x, axis=-1, keepdims=True) * (1.0 / width)
        cen = x - mean
        var = jnp.sum(cen * cen, axis=-1, keepdims=True) * (1.0 / width)
        inv = lax.rsqrt(var + LN_EPS)
        hat = jnp.sum(cen * inv, axis=0) * (1.0 / tokens)
        xm[pl.ds(row0, pb), :] = hat
        pf[0, pl.ds(row0, pb), :] = (hat * gam_ref[...] + bet_ref[...]).astype(BF16).astype(F32)
        blk = row0 // 8
        ids = lane_ids((tokens, 8, LANES))
        st_ref[...] = jnp.where(ids == blk, mean, jnp.where(ids == blk + 64, inv, st_ref[...]))

    def norm_chunk(j, prefetch):
        slot = lax.rem(j, nslot)
        for c in fetch(j):
            c.wait()

        def one(h, _):
            norm_rows(slot, h, pl.multiple_of(jnp.where(h == 0, arow(j), brow(j)), 8))
            return 0

        lax.fori_loop(0, 2, one, 0)
        if prefetch:
            for c in fetch(j + nslot):
                c.start()

    def norm_chunks(lo, hi):
        for a, b, pre in ((lo, min(hi, npl - nslot), True), (max(lo, npl - nslot), hi, False)):
            if b > a:
                lax.fori_loop(a, b, lambda j, _, pre=pre: (norm_chunk(j, pre), 0)[1], 0)

    dcols, pcols = pl.ds(0, direct), pl.ds(direct, width - direct)

    def straight(j):
        out = []
        for d, x in xpeer:
            for rows in (arow(j), brow(j)):
                rows = pl.ds(rows, pb)
                out.append(remote(pf.at[0, rows, dcols], pf.at[nx - d, rows, dcols], xd_send.at[d - 1], xd_recv.at[nx - d - 1], dev(x=x)))
        return out

    def send_straight(j):
        for c in straight(j):
            c.start()

    def norm_and_send(lo, hi):
        for a, b, pre in ((lo, min(hi, npl - nslot), True), (max(lo, npl - nslot), hi, False)):
            if b > a:
                lax.fori_loop(a, b, lambda j, _, pre=pre: (norm_chunk(j, pre), send_straight(j), 0)[2], 0)

    first = min(3, npl // 2)
    cuts = [first, npl // 2, npl * 13 // 16]
    norm_chunks(0, first)

    def pack_labels(g, acc):
        for k in range(8):
            acc = jnp.where((lane8 == g) & (row8 == k), lab_ref[g * 8 + k].astype(F32), acc)
        return acc

    labs[0] = lax.fori_loop(0, groups, pack_labels, jnp.zeros((8, LANES), F32))
    pl.semaphore_wait(barrier, len(everyone))

    own_a, own_b = pl.ds(arow(0), pb), pl.ds(brow(0), pb)
    order = sorted(range(1, nx), key=lambda slot: min(slot, nx - slot))
    xs = {}
    for d, x in sorted(xpeer, key=lambda dx: min(dx[0], nx - dx[0])):
        xs[nx - d] = []
        for k, rows in enumerate((own_a, own_b)):
            xs[nx - d].append(remote(pf.at[0, rows, pcols], pf.at[nx - d, rows, pcols], x_send.at[nx - d - 1, k], x_recv.at[nx - d - 1, k], dev(x=x)))
        xs[nx - d].append(remote(labs.at[0], labs.at[nx - d], xl_send.at[nx - d - 1], xl_recv.at[nx - d - 1], dev(x=x)))
        for c in xs[nx - d]:
            c.start()
    lax.fori_loop(0, first, lambda j, _: (send_straight(j), 0)[1], 0)
    norm_and_send(first, cuts[1])

    blk_a = pl.ds(pl.multiple_of(zi * za, 8), za)
    blk_b = pl.ds(pl.multiple_of(half + yi * ya, 8), ya)
    g1, g2 = {}, {}
    for slot in order:
        for c in xs[slot]:
            c.wait()
        g1[slot] = []
        for k, peers, n, rows in ((0, [(d, dev(y=y)) for d, y in ypeer], ny, own_a), (1, [(d, dev(z=z)) for d, z in zpeer], nz, own_b)):
            for d, who in peers:
                ref = pf.at[slot, rows, pcols]
                g1[slot].append(remote(ref, ref, g_send.at[k, slot - 1, d - 1], g_recv.at[k, slot - 1, n - d - 1], who))
        for c in g1[slot]:
            c.start()
    norm_and_send(cuts[1], cuts[2])
    for slot in order:
        for c in g1[slot]:
            c.wait()
        g2[slot] = []
        for k, peers, n, rows in ((2, [(d, dev(z=z)) for d, z in zpeer], nz, blk_a), (3, [(d, dev(y=y)) for d, y in ypeer], ny, blk_b)):
            for d, who in peers:
                ref = pf.at[slot, rows, pcols]
                g2[slot].append(remote(ref, ref, g_send.at[k, slot - 1, d - 1], g_recv.at[k, slot - 1, n - d - 1], who))
        for c in g2[slot]:
            c.start()
    norm_and_send(cuts[2], npl)
    w_copy.wait()

    col = (tp * cols + lane_ids((1, cols))).astype(F32)
    valid = col < float(VALID_CLASSES)
    vweight = jnp.where(valid, SMOOTH / VALID_CLASSES, 0.0)
    sub = min(64, ti)

    def col_of(packed, lane):
        return jnp.sum(jnp.where(lane8 == lane, packed, 0.0), axis=-1, keepdims=True)

    def cols_of(packed, lane):
        return jnp.concatenate([col_of(packed, lane + k) for k in range(sub // 8)], axis=0)

    near[tp] = jnp.zeros_like(near[0])
    stat[tp] = jnp.zeros_like(stat[0])
    bias = b_ref[...].reshape(1, cols)

    def logits_of(slot, out):
        xabs = lax.rem(xi + slot, nx)
        p16[xabs] = pf[slot].astype(BF16)
        lt[...] = jnp.dot(p16[xabs], w[...], preferred_element_type=F32)

        def body(r, carry):
            ms, ss, pp = carry
            rows = pl.ds(pl.multiple_of(r * sub, sub), sub)
            l = jnp.where(valid, lt[rows, :] + bias, -1e30)
            m = jnp.max(l, axis=-1, keepdims=True)
            e = jnp.exp(l - m)
            s = jnp.sum(e, axis=-1, keepdims=True)
            lg[xabs, rows, :] = e
            hot = col == cols_of(labs[slot], r * (sub // 8))
            ps = jnp.sum(jnp.where(hot, vweight + (1.0 - SMOOTH), vweight) * l, axis=-1, keepdims=True)
            for k in range(sub // 8):
                here = lane8 == xabs * groups + r * (sub // 8) + k
                ms = jnp.where(here, m[8 * k : 8 * k + 8], ms)
                ss = jnp.where(here, s[8 * k : 8 * k + 8], ss)
                pp = jnp.where(here, ps[8 * k : 8 * k + 8], pp)
            return ms, ss, pp

        ms, ss, pp = lax.fori_loop(0, ti // sub, body, (out[tp, 0], out[tp, 1], stat[tp, 2]))
        out[tp, 0], out[tp, 1], stat[tp, 2] = ms, ss, pp

    def gathered(slot):
        for c in g2[slot]:
            c.wait()
        ref = pf.at[slot, :, dcols]
        remote(ref, ref, xd_send.at[nx - slot - 1], xd_recv.at[slot - 1], dev(x=xpeer[slot - 1][1])).wait_recv()
        logits_of(slot, stat)

    def merged(buf, used):
        m = buf[0, 0]
        for k in range(1, npl):
            m = jnp.maximum(m, buf[k, 0])
        s = jnp.zeros_like(m)
        for k in range(npl):
            s = s + buf[k, 1] * jnp.exp(buf[k, 0] - m)
        coef = jnp.where(used, jnp.exp(buf[tp, 0] - m) / s * (1.0 / rows_total), 0.0)
        return coef, jnp.where(used, m + jnp.log(jnp.where(used, s, 1.0)), 0.0)

    vscaled = vweight * (1.0 / rows_total)
    vhot = vscaled + (1.0 - SMOOTH) / rows_total

    def dlogit_of(slot):
        xabs = lax.rem(xi + slot, nx)

        def body(r, acc):
            rows = pl.ds(pl.multiple_of(r * sub, sub), sub)
            cf = cols_of(cof[...], xabs * groups + r * (sub // 8))
            hot = col == cols_of(labs[slot], r * (sub // 8))
            dl = lg[xabs, rows, :] * cf - jnp.where(hot, vhot, vscaled)
            dl16[xabs, rows, :] = dl.astype(BF16)
            return acc + jnp.sum(dl.reshape(sub // 8, 8, cols), axis=0)

        dbs[xabs] = lax.fori_loop(0, ti // sub, body, jnp.zeros((8, cols), F32))

    lane_block = lane8 // groups
    logits_of(0, near)
    st0 = [remote(near.at[tp], near.at[tp], n_send.at[k - 1], n_recv.at[k - 1], who) for k, who in plane]
    for c in st0:
        c.start()
    gathered(order[0])
    for c in st0:
        c.wait()
    coef, lse0 = merged(near, lane_block == xi)
    cof[...] = coef
    dlogit_of(0)
    dpp[...] = lax.dot_general(dl16[xi], w[...], (((1,), (1,)), ((), ())), preferred_element_type=F32)

    r1 = []
    for d, z in zpeer:
        r1.append(remote(dpp.at[pl.ds(pl.multiple_of(z * za, 8), za)], ra.at[nz - d - 1], r_send.at[0, d - 1], r_recv.at[0, nz - d - 1], dev(z=z)))
    for d, y in ypeer:
        r1.append(remote(dpp.at[pl.ds(pl.multiple_of(half + y * ya, 8), ya)], rb.at[ny - d - 1], r_send.at[1, d - 1], r_recv.at[1, ny - d - 1], dev(y=y)))
    for c in r1:
        c.start()
    for slot in order[1:]:
        gathered(slot)
    st1 = [remote(stat.at[tp], stat.at[tp], s_send.at[k - 1], s_recv.at[k - 1], who) for k, who in plane]
    for c in st1:
        c.start()
    for slot in order:
        ref = pf.at[slot, :, dcols]
        remote(ref, ref, xd_send.at[slot - 1], xd_recv.at[slot - 1], dev(x=xpeer[slot - 1][1])).wait_send()

    for c in r1:
        c.wait()

    def total(buf, own, n):
        t = own
        for k in range(n - 1):
            t = t + buf[k]
        return t

    ta[...] = total(ra, dpp[blk_a, :], nz)
    tb[...] = total(rb, dpp[blk_b, :], ny)
    r2 = []
    for d, y in ypeer:
        r2.append(remote(ta.at[pl.ds(pl.multiple_of(y * pb, 8), pb)], ra2.at[ny - d - 1], r_send.at[2, d - 1], r_recv.at[2, ny - d - 1], dev(y=y)))
    for d, z in zpeer:
        r2.append(remote(tb.at[pl.ds(pl.multiple_of(z * pb, 8), pb)], rb2.at[nz - d - 1], r_send.at[3, d - 1], r_recv.at[3, nz - d - 1], dev(z=z)))
    for c in r2:
        c.start()

    mh = width // 2

    def dw_half(h, out):
        lhs_cols = pl.ds(pl.multiple_of(h * mh, 128), mh)
        k = nx * ti
        out[...] = lax.dot_general(p16[:, :, lhs_cols].reshape(k, mh), dl16[...].reshape(k, cols), (((0,), (0,)), ((), ())), preferred_element_type=F32)

    for c in r2:
        c.wait()
    dpf[own_a, :] = total(ra2, ta[pl.ds(pl.multiple_of(yi * pb, 8), pb), :], ny)
    dpf[own_b, :] = total(rb2, tb[pl.ds(pl.multiple_of(zi * pb, 8), pb), :], nz)
    gy[yi, 0:1, :] = jnp.sum(dpf[own_a, :] * xm[own_a, :] + dpf[own_b, :] * xm[own_b, :], axis=0, keepdims=True)
    gy[yi, 1:2, :] = jnp.sum(dpf[own_a, :] + dpf[own_b, :], axis=0, keepdims=True)
    a1 = []
    for d, y in ypeer:
        a1.append(remote(dpf.at[own_a], dpf.at[own_a], r_send.at[4, d - 1], r_recv.at[4, ny - d - 1], dev(y=y)))
    for d, z in zpeer:
        a1.append(remote(dpf.at[own_b], dpf.at[own_b], r_send.at[5, d - 1], r_recv.at[5, nz - d - 1], dev(z=z)))
    for d, y in ypeer:
        a1.append(remote(gy.at[yi], gy.at[yi], q_send.at[0, d - 1], q_recv.at[0, ny - d - 1], dev(y=y)))
    for c in a1:
        c.start()
    for c in st1:
        c.wait()
    coef, lse1 = merged(stat, (lane_block != xi) & (lane_block < nx))
    loss_rows = lse0 + lse1
    for k in range(npl):
        loss_rows = loss_rows - stat[k, 2]
    cof[...] = coef
    dlogit_of(order[0])
    for c in a1:
        c.wait()
    a2 = []
    for d, z in zpeer:
        a2.append(remote(dpf.at[blk_a], dpf.at[blk_a], r_send.at[6, d - 1], r_recv.at[6, nz - d - 1], dev(z=z)))
    for d, y in ypeer:
        a2.append(remote(dpf.at[blk_b], dpf.at[blk_b], r_send.at[7, d - 1], r_recv.at[7, ny - d - 1], dev(y=y)))

    def summed(buf, n):
        t = buf[0]
        for k in range(1, n):
            t = t + buf[k]
        return t

    gz[zi] = summed(gy, ny)
    t1 = [remote(gz.at[zi], gz.at[zi], q_send.at[1, d - 1], q_recv.at[1, nz - d - 1], dev(z=z)) for d, z in zpeer]
    for c in t1 + a2:
        c.start()
    for slot in order[1:]:
        dlogit_of(slot)
    dw_half(1 - ci, dwpart)
    ex = remote(dwpart, dwrecv, d_send.at[0], d_recv.at[0], dev(c=1 - ci))
    ex.start()
    dw_half(ci, dwbuf.at[0])
    for c in t1:
        c.wait()
    gx[xi] = summed(gz, nz)
    t2 = [remote(gx.at[xi], gx.at[xi], q_send.at[2, d - 1], q_recv.at[2, nx - d - 1], dev(x=x)) for d, x in xpeer]
    for c in t2:
        c.start()
    ex.wait()
    dwbuf[0] = dwbuf[0] + dwrecv[...]
    back = remote(dwbuf.at[0], dwbuf.at[1], d_send.at[1], d_recv.at[1], dev(c=1 - ci))
    back.start()
    gc[0] = jnp.zeros_like(gc[0])
    gc[0, 0:1, width : width + cols] = jnp.sum(summed(dbs, nx), axis=0, keepdims=True)
    gc[0, :, width + cols :] = loss_rows
    for c in t2:
        c.wait()
    gc[0, :, 0:width] = summed(gx, nx)
    t3 = remote(gc.at[0], gc.at[1], q_send.at[3, 0], q_recv.at[3, 0], dev(c=1 - ci))
    t3.start()
    for c in a2:
        c.wait()
    t3.wait()
    small_ref[...] = gc[0] + gc[1]
    back.wait()


def norm_bwd_kernel(rows_total, f_ref, dp_ref, gam_ref, st_ref, dwin_ref, small_ref, out_ref, dw_ref, loss_ref, db_ref, dg_ref, dbt_ref):
    tokens, rows, width = f_ref.shape
    cols = db_ref.shape[0]
    i = pl.program_id(0)
    ids = lane_ids((tokens, 8, LANES))

    def one(h, _):
        r = pl.ds(pl.multiple_of(h * 8, 8), 8)
        blk = i * (rows // 8) + h
        u = dp_ref[r, :] * gam_ref[...] * (1.0 / tokens)
        ut = u - jnp.mean(u, axis=-1, keepdims=True)
        st = st_ref[...]
        mean = jnp.sum(jnp.where(ids == blk, st, 0.0), axis=-1, keepdims=True)
        inv = jnp.sum(jnp.where(ids == blk + 64, st, 0.0), axis=-1, keepdims=True)
        cen = f_ref[:, r, :].astype(F32) - mean
        proj = jnp.sum(cen * ut[None], axis=-1, keepdims=True) * inv * (1.0 / width)
        out_ref[:, r, :] = (inv * (ut[None] - cen * (inv * proj))).astype(BF16)
        return 0

    lax.fori_loop(0, rows // 8, one, 0)
    dr = dw_ref.shape[0]
    per = width // 2 // dr
    own = (i // per) == lax.rem(lax.axis_index("dp"), 2)
    dw_ref[...] = dwin_ref[jnp.where(own, 0, 1), pl.ds(pl.multiple_of(lax.rem(i, per) * dr, 8), dr), :]

    @pl.when(i == 0)
    def _():
        dg_ref[...] = small_ref[0:1, 0:width].reshape(width)
        dbt_ref[...] = small_ref[1:2, 0:width].reshape(width)
        db_ref[...] = small_ref[0:1, width : width + cols].reshape(cols)
        tail = jnp.sum(jnp.sum(small_ref[:, width + cols :], axis=-1, keepdims=True), axis=0, keepdims=True)
        loss_ref[...] = tail * (1.0 / rows_total)


def solution(mesh):
    sides = SIDES[mesh.devices.size]
    nx, ny, nz = sides
    dp_size = mesh.shape["dp"]

    def local_head(feats, ln_gamma, ln_beta, w_head, b_head, labels):
        ti, tokens, width = feats.shape
        cols = w_head.shape[1]
        half = ti // 2
        pb = half // (ny * nz)
        ft = jnp.transpose(feats, (1, 0, 2))
        gam, bet = ln_gamma[None], ln_beta[None]
        vm = pl.BlockSpec(memory_space=pltpu.VMEM)
        hbm = pl.BlockSpec(memory_space=pl.ANY)
        sm = pl.BlockSpec(memory_space=pltpu.SMEM)
        sem = pltpu.SemaphoreType.DMA
        n3 = max(nx, ny, nz)
        npl = ny * nz
        S = jax.ShapeDtypeStruct
        extra = width + cols + LANES
        dw, small, dpool, st = pl.pallas_call(
            functools.partial(head_kernel, sides, ti * dp_size),
            out_shape=(pltpu.VMEM((2, width // 2, cols), F32), pltpu.VMEM((8, extra), F32), pltpu.VMEM((ti, width), F32), pltpu.VMEM((tokens, 8, LANES), F32)),
            in_specs=[hbm, vm, vm, hbm, vm, sm],
            out_specs=(vm, vm, vm, vm),
            scratch_shapes=[
                pltpu.VMEM((min(4, npl), 2, tokens, pb, width), BF16),
                pltpu.VMEM((width, cols), BF16),
                pltpu.VMEM((nx, ti, width), F32),
                pltpu.VMEM((nx, ti, width), BF16),
                pltpu.VMEM((ti, cols), F32),
                pltpu.VMEM((nx, ti, cols), F32),
                pltpu.VMEM((nx, ti, cols), BF16),
                pltpu.VMEM((width // 2, cols), F32),
                pltpu.VMEM((width // 2, cols), F32),
                pltpu.VMEM((ti, width), F32),
                pltpu.VMEM((ti, width), F32),
                pltpu.VMEM((nx, 8, LANES), F32),
                pltpu.VMEM((nz - 1, half // nz, width), F32),
                pltpu.VMEM((ny - 1, half // ny, width), F32),
                pltpu.VMEM((ny - 1, pb, width), F32),
                pltpu.VMEM((nz - 1, pb, width), F32),
                pltpu.VMEM((half // nz, width), F32),
                pltpu.VMEM((half // ny, width), F32),
                pltpu.VMEM((npl, 2, 8, LANES), F32),
                pltpu.VMEM((npl, 3, 8, LANES), F32),
                pltpu.VMEM((8, LANES), F32),
                pltpu.VMEM((nx, 8, cols), F32),
                pltpu.VMEM((ny, 8, width), F32),
                pltpu.VMEM((nz, 8, width), F32),
                pltpu.VMEM((nx, 8, width), F32),
                pltpu.VMEM((2, 8, extra), F32),
                sem((min(4, npl), 2)),
                sem,
                sem((nx - 1, 2)), sem((nx - 1, 2)), sem((nx - 1,)), sem((nx - 1,)), sem((nx - 1,)), sem((nx - 1,)),
                sem((4, nx - 1, n3 - 1)), sem((4, nx - 1, n3 - 1)),
                sem((npl - 1,)), sem((npl - 1,)), sem((npl - 1,)), sem((npl - 1,)),
                sem((8, n3 - 1)), sem((8, n3 - 1)),
                sem((2,)), sem((2,)),
                sem((4, n3 - 1)), sem((4, n3 - 1)),
            ],
            compiler_params=pltpu.CompilerParams(collective_id=0, has_side_effects=True, vmem_limit_bytes=50 * 1024 * 1024),
        )(ft, gam, bet, w_head, b_head, labels)
        rb = 16
        steps = ti // rb
        near = lambda a: pltpu.with_memory_space_constraint(a, pltpu.VMEM)
        dft, dwo, loss, db, dg, dbt = pl.pallas_call(
            functools.partial(norm_bwd_kernel, ti * dp_size),
            grid=(steps,),
            out_shape=(S((tokens, ti, width), BF16), S((width, cols), F32), S((1, 1), F32), S((cols,), F32), S((width,), F32), S((width,), F32)),
            in_specs=[
                pl.BlockSpec((tokens, rb, width), lambda i: (0, i, 0)),
                pl.BlockSpec((rb, width), lambda i: (i, 0)),
                pl.BlockSpec((1, width), lambda i: (0, 0)),
                vm, vm, vm,
            ],
            out_specs=(
                pl.BlockSpec((tokens, rb, width), lambda i: (0, i, 0)),
                pl.BlockSpec((width // steps, cols), lambda i: (i, 0)),
                vm, vm, vm, vm,
            ),
            compiler_params=pltpu.CompilerParams(vmem_limit_bytes=40 * 1024 * 1024),
        )(ft, dpool, gam, near(st), near(dw), near(small))
        return loss[0, 0], jnp.transpose(dft, (1, 0, 2)), dwo, db, dg, dbt

    return jax.shard_map(
        local_head,
        mesh=mesh,
        in_specs=(P("dp", None, None), P(), P(), P(None, "tp"), P("tp"), P("dp")),
        out_specs=(P(), P("dp", None, None), P(None, "tp"), P("tp"), P(), P()),
        check_vma=False,
    )
```
